32 devices in a mesh: dp: 8 (over z, y), tensor: 4 (over x, core).
Axes of the slice: x: 2, y: 2, z: 4, core: 2. Of those that a mesh axis runs over, the one named last changes fastest.
Arguments:
- tokens: bfloat16 [16384, 1536], P('dp', 'tensor'), may hold values from -6 to 6
- segments: int32 [16384], P('dp'), may hold values from 0 to 5, as said below
- prenorm: float32 [1536], replicated, may hold values from 0.5 to 1.5
- gating: bfloat16 [1536, 3072], P(None, 'tensor'), may hold values from -0.15625 to 0.15625
- signal: bfloat16 [1536, 3072], P(None, 'tensor'), may hold values from -0.15625 to 0.15625
- memory: bfloat16 [1536, 256], replicated, may hold values from -0.15625 to 0.15625
- timestep: bfloat16 [1536, 48], P(None, 'tensor'), may hold values from -0.15625 to 0.15625
- kernel: float32 [4, 3072], P(None, 'tensor'), may hold values from -3 to 3
- offsets: float32 [3072], P('tensor'), may hold values from -0.5 to 0.5
- window: float32 [4, 256], replicated, may hold values from -3 to 3
- shifts: float32 [256], replicated, may hold values from -0.5 to 0.5
- baseline: float32 [48], P('tensor'), may hold values from -6.9 to -2.3
- decays: float32 [48], P('tensor'), may hold values from 0 to 2.77
- shortcut: float32 [48], P('tensor'), may hold values from 0.5 to 1.5
- postnorm: float32 [3072], P('tensor'), may hold values from 0.5 to 1.5
- readout: bfloat16 [3072, 1536], P('tensor'), may hold values from -0.109375 to 0.109375
- cotangent: bfloat16 [16384, 1536], P('dp', 'tensor'), may hold values from -6 to 6
Outputs:
- result: bfloat16 [16384, 1536], P('dp', 'tensor')
- tokens_gradient: float32 [16384, 1536], P('dp', 'tensor')
- prenorm_gradient: float32 [1536], P('tensor')
- gating_gradient: float32 [1536, 3072], P(None, 'tensor')
- signal_gradient: float32 [1536, 3072], P(None, 'tensor')
- memory_gradient: float32 [1536, 256], P('tensor')
- timestep_gradient: float32 [1536, 48], P(None, 'tensor')
- kernel_gradient: float32 [4, 3072], P(None, 'tensor')
- offsets_gradient: float32 [3072], P('tensor')
- window_gradient: float32 [4, 256], replicated
- shifts_gradient: float32 [256], replicated
- baseline_gradient: float32 [48], P('tensor')
- decays_gradient: float32 [48], P('tensor')
- shortcut_gradient: float32 [48], P('tensor')
- postnorm_gradient: float32 [3072], P('tensor')
- readout_gradient: float32 [3072, 1536], P('tensor')
The draws below stay inside these ranges and needn't reach their ends.
Inputs may be any that keep to these rules, and one draw needn't show every extreme that they name: `segments`: within each sequence of 1024 consecutive tokens the numbers start at 0 and rise by one where a new document starts; documents hold 200 to 1000 tokens, except that the last one of a sequence may be shorter.
All inputs are finite; a program needn't handle non-finite values.
Results may differ from the reference program's by a relative error of at most 0.0082.
Values may be sent and summed in bfloat16 or wider, within the bound.
A program may use at most 384 MiB of HBM per device.

```python
import jax
import jax.numpy as jnp
from jax import lax

D = 1536
HEADS = 48
STATE = 128
CONV = 4
SPAN = 256
SEQLEN = 1024
DOC_MIN = 200
DOC_MAX = 1000
INNER = 3072
SEQS = 16
TOKENS = 16384


def draw_segments(key, part):
    most_docs = SEQLEN // DOC_MIN + 1
    length_key = jax.random.fold_in(key, 11)
    pick_key = jax.random.fold_in(key, 23)
    lengths = jax.random.randint(length_key, (SEQS, most_docs), DOC_MIN, DOC_MAX + 1)
    chosen = jax.random.randint(pick_key, (), 0, SEQS)
    shortest = (jnp.arange(SEQS, dtype=jnp.int32) == chosen)[:, None]
    lengths = jnp.where(shortest, DOC_MIN, lengths).astype(jnp.int32)
    closing = jnp.cumsum(lengths, axis=1)
    places = jnp.arange(SEQLEN, dtype=jnp.int32)
    counted = jnp.sum((closing[:, None, :] <= places[None, :, None]).astype(jnp.int32), axis=-1)
    return counted.reshape(SEQS * SEQLEN).astype(jnp.int32)


def block_levels(key, shape, pieces, least, top_value):
    level = 1.0
    for position, parts in pieces:
        steps = jax.random.uniform(jax.random.fold_in(jax.random.fold_in(key, 6), position), (parts,), jnp.float32, least / len(pieces), top_value / len(pieces))
        level = level * jnp.repeat(jnp.exp(steps), shape[position] // parts).reshape((-1,) + (1,) * (len(shape) - 1 - position))
    return level


def gaussian(stream_key, dims, width, reach, cuts=(), held_as=jnp.bfloat16):
    level = block_levels(stream_key, dims, cuts, -0.22, 0.18) if cuts else 1.0
    values = jax.random.normal(stream_key, dims, jnp.float32) * width * level
    return jnp.minimum(jnp.maximum(values, -reach), reach).astype(held_as)


def setup_inputs(seed: int = 0) -> dict:
    key_of = jax.random.split(jax.random.key(seed), 18)
    tokens = gaussian(key_of[0], (TOKENS, D), 1.0, 6.0, ((0, 8), (1, 4)))
    segments = draw_segments(jax.random.fold_in(key_of[17], 71), 0)
    prenorm = jnp.clip(1.0 + 0.1 * jax.random.normal(key_of[2], (D,), jnp.float32), 0.5, 1.5)
    gating = gaussian(key_of[3], (D, INNER), D ** -0.5, 0.15625, ((1, 4),))
    signal = gaussian(key_of[4], (D, INNER), D ** -0.5, 0.15625, ((1, 4),))
    memory = gaussian(key_of[5], (D, 2 * STATE), D ** -0.5, 0.15625)
    timestep = gaussian(key_of[6], (D, HEADS), D ** -0.5, 0.15625, ((1, 4),))
    kernel = gaussian(key_of[7], (CONV, INNER), CONV ** -0.5, 3.0, ((1, 4),), jnp.float32)
    offsets = jnp.clip(jax.random.uniform(key_of[8], (INNER,), jnp.float32, -0.5, 0.5) * block_levels(key_of[8], (INNER,), ((0, 4),), -0.4, 0.0), -0.5, 0.5)
    window = gaussian(key_of[9], (CONV, 2 * STATE), CONV ** -0.5, 3.0, (), jnp.float32)
    shifts = jnp.clip(jax.random.uniform(key_of[10], (2 * STATE,), jnp.float32, -0.5, 0.5), -0.5, 0.5)
    baseline = jnp.clip(-6.9 + 4.6000001430511475 * jax.random.uniform(key_of[11], (HEADS,), jnp.float32) ** block_levels(key_of[11], (HEADS,), ((0, 4),), -0.2, 0.2), -6.9, -2.3)
    decays = jnp.clip(2.77 * jax.random.uniform(key_of[12], (HEADS,), jnp.float32) ** block_levels(key_of[12], (HEADS,), ((0, 4),), -0.2, 0.2), 0.0, 2.77)
    shortcut = jnp.clip(1.0 + 0.1 * jax.random.normal(key_of[13], (HEADS,), jnp.float32), 0.5, 1.5)
    postnorm = jnp.clip(1.0 + 0.1 * jax.random.normal(key_of[14], (INNER,), jnp.float32), 0.5, 1.5)
    readout = gaussian(key_of[15], (INNER, D), INNER ** -0.5, 0.109375, ((0, 4),))
    cotangent = gaussian(key_of[16], (TOKENS, D), 1.0, 6.0, ((0, 8), (1, 4)))
    return dict(tokens=tokens, segments=segments, prenorm=prenorm, gating=gating, signal=signal, memory=memory, timestep=timestep, kernel=kernel, offsets=offsets, window=window, shifts=shifts, baseline=baseline, decays=decays, shortcut=shortcut, postnorm=postnorm, readout=readout, cotangent=cotangent)


epsilon = 1e-05
highest = lax.Precision.HIGHEST

@jax.custom_vjp
def low(v):
    return lax.optimization_barrier(v.astype(jnp.bfloat16)).astype(jnp.float32)

@jax.custom_vjp
def low_back(v):
    return v

def low_keep(v):
    return (low(v), None)

def low_pass(kept, grad):
    return (grad,)

def back_keep(v):
    return (v, None)

def back_low(kept, grad):
    return (low(grad),)
low.defvjp(low_keep, low_pass)
low_back.defvjp(back_keep, back_low)

def causal_filter(values, weight, offset, segment):
    length = values.shape[1]
    summed = offset + weight[0] * values
    for lag_steps in range(1, weight.shape[0]):
        shifted = jnp.pad(values, ((0, 0), (lag_steps, 0), (0, 0)))[:, :length]
        earlier = jnp.pad(segment, ((0, 0), (lag_steps, 0)), constant_values=-1)[:, :length]
        matched = (earlier == segment).astype(jnp.float32)[:, :, None]
        summed = summed + weight[lag_steps] * shifted * matched
    return summed

def span_scan(signal_heads, stepsize, logdecay, writes, reads, segment):
    batches = signal_heads.shape[0]
    length = signal_heads.shape[1]
    heads_here = signal_heads.shape[2]
    head_width = signal_heads.shape[3]
    state_width = writes.shape[-1]
    blocks = length // SPAN

    def into_blocks(member):
        return jnp.swapaxes(member.reshape((batches, blocks, SPAN) + member.shape[2:]), 0, 1)
    lower_part = jnp.tril(jnp.ones((SPAN, SPAN), dtype=bool))

    def advance(carried_in, block_data):
        memory_state, last_segment = carried_in
        piece_signal, piece_step, piece_decay, piece_write, piece_read, piece_segment = block_data
        running = jnp.cumsum(piece_decay, axis=1)
        inside = lower_part[None] & (piece_segment[:, :, None] == piece_segment[:, None, :])
        inside_heads = inside[:, :, :, None]
        spread = running[:, :, None, :] - running[:, None, :, :]
        falloff = jnp.where(inside_heads, jnp.exp(jnp.where(inside_heads, spread, 0.0)), 0.0)
        scores = jnp.einsum('btn,bsn->bts', piece_read, piece_write, precision=highest)
        mixing = falloff * scores[:, :, :, None] * piece_step[:, None, :, :]
        output = jnp.einsum('btsh,bshp->bthp', mixing, piece_signal, precision=highest)
        carried = (piece_segment == last_segment[:, None]).astype(jnp.float32)
        entering = jnp.exp(running) * carried[:, :, None]
        output = output + jnp.einsum('btn,bhpn->bthp', piece_read, memory_state, precision=highest) * entering[:, :, :, None]
        tail_segment = piece_segment[:, -1]
        keeping = (piece_segment == tail_segment[:, None]).astype(jnp.float32)
        toward = jnp.exp(running[:, -1:, :] - running) * keeping[:, :, None] * piece_step
        persist = jnp.exp(running[:, -1, :]) * (tail_segment == last_segment).astype(jnp.float32)[:, None]
        memory_state = memory_state * persist[:, :, None, None] + jnp.einsum('bsh,bshp,bsn->bhpn', toward, piece_signal, piece_write, precision=highest)
        return ((memory_state, tail_segment), output)
    starting = (jnp.zeros((batches, heads_here, head_width, state_width), jnp.float32), jnp.full((batches,), -1, jnp.int32))
    block_inputs = (into_blocks(signal_heads), into_blocks(stepsize), into_blocks(logdecay), into_blocks(writes), into_blocks(reads), into_blocks(segment))
    finished, outputs = lax.scan(advance, starting, block_inputs)
    return jnp.swapaxes(outputs, 0, 1).reshape(batches, length, heads_here, head_width)

def mixer(segment, gate_in, signal_in, memory_in, step_in, kernel, offsets, window, shifts, baseline, decays, shortcut):
    batches = segment.shape[0]
    length = segment.shape[1]
    signal_seq = jax.nn.silu(causal_filter(signal_in.reshape(batches, length, -1), kernel, offsets, segment))
    memory_seq = jax.nn.silu(causal_filter(memory_in.reshape(batches, length, -1), window, shifts, segment))
    state_width = memory_seq.shape[-1] // 2
    writes = memory_seq[..., :state_width]
    reads = memory_seq[..., state_width:]
    stepsize = jax.nn.softplus(step_in.reshape(batches, length, -1) + baseline)
    logdecay = -jnp.exp(decays) * stepsize
    heads_here = stepsize.shape[-1]
    signal_heads = signal_seq.reshape(batches, length, heads_here, -1)
    scanned = span_scan(signal_heads, stepsize, logdecay, writes, reads, segment) + shortcut[:, None] * signal_heads
    return scanned.reshape(batches * length, -1) * jax.nn.silu(gate_in)

def layer(weights, rows, segment):
    prenorm, gating, signal, memory, timestep, kernel, offsets, window, shifts, baseline, decays, shortcut, postnorm, readout = weights
    scale = lax.rsqrt(lax.optimization_barrier(jnp.mean(rows * rows, axis=-1, keepdims=True)) + epsilon)
    normed = low(rows * scale * prenorm)
    gate_in = low_back(jnp.dot(normed, gating, precision=highest))
    signal_in = low_back(jnp.dot(normed, signal, precision=highest))
    memory_in = low_back(jnp.dot(normed, memory, precision=highest))
    step_in = low_back(jnp.dot(normed, timestep, precision=highest))
    gated = mixer(segment[None], gate_in, signal_in, memory_in, step_in, kernel, offsets, window, shifts, baseline, decays, shortcut)
    factor = lax.rsqrt(lax.optimization_barrier(jnp.mean(gated * gated, axis=-1, keepdims=True)) + epsilon)
    outnormed = low(gated * factor * postnorm)
    return rows + jnp.dot(outnormed, readout, precision=highest)

def reference(tokens, segments, prenorm, gating, signal, memory, timestep, kernel, offsets, window, shifts, baseline, decays, shortcut, postnorm, readout, cotangent):
    params = tuple((member.astype(jnp.float32) for member in (prenorm, gating, signal, memory, timestep, kernel, offsets, window, shifts, baseline, decays, shortcut, postnorm, readout)))
    segment_rows = segments.reshape(SEQS, SEQLEN).astype(jnp.int32)

    def forward(tokens_wide, weights):

        def one_sequence(paired):
            return layer(weights, paired[0], paired[1])
        outputs = lax.map(jax.checkpoint(one_sequence), (tokens_wide.reshape(SEQS, SEQLEN, D), segment_rows))
        return outputs.reshape(TOKENS, D)
    outcome, pull = jax.vjp(forward, tokens.astype(jnp.float32), params)
    tokens_grad, weight_grads = pull(cotangent.astype(jnp.float32))
    return (outcome.astype(jnp.bfloat16), tokens_grad, weight_grads[0], weight_grads[1], weight_grads[2], weight_grads[3], weight_grads[4], weight_grads[5], weight_grads[6], weight_grads[7], weight_grads[8], weight_grads[9], weight_grads[10], weight_grads[11], weight_grads[12], weight_grads[13])
```

```python
from functools import partial

import jax
import jax.numpy as jnp
from jax import lax
from jax.experimental import pallas as pl
from jax.experimental.pallas import tpu as pltpu
from jax.sharding import PartitionSpec as P

SEQLEN = 1024
CHUNK = 128
LANES = 128
HALO = 8
LOG2E = 1.4426950408889634
epsilon = 1e-05
f32 = jnp.float32
bf16 = jnp.bfloat16


def dot_nn(a, b):
    return lax.dot_general(a, b, (((1,), (0,)), ((), ())), preferred_element_type=f32)


def dot_nt(a, b):
    return lax.dot_general(a, b, (((1,), (1,)), ((), ())), preferred_element_type=f32)


def dot_tn(a, b):
    return lax.dot_general(a, b, (((0,), (0,)), ((), ())), preferred_element_type=f32)


def halves(v):
    hi = v.astype(bf16)
    lo = (v - hi.astype(f32)).astype(bf16)
    return hi, lo


def spread_heads(v, twice):
    hi, lo = halves(v)
    return dot_nn(jnp.concatenate([hi, lo], axis=1), twice)


def sum_heads(v, once):
    hi, lo = halves(v)
    return dot_nt(hi, once) + dot_nt(lo, once)


def tri_dot(tri, v):
    hi = v.astype(bf16)
    rest = v - hi.astype(f32)
    mid = rest.astype(bf16)
    lo = (rest - mid.astype(f32)).astype(bf16)
    return dot_nn(tri, hi) + (dot_nn(tri, mid) + dot_nn(tri, lo))


def softplus(v):
    return jnp.maximum(v, 0.0) + jnp.log1p(jnp.exp(-jnp.abs(v)))


def precise_nt(a, b):
    ah, al = halves(a)
    bh, bl = halves(b)
    return dot_nt(jnp.concatenate([ah, ah, al], axis=1), jnp.concatenate([bh, bl, bh], axis=1))


def filtered(ext, value, halo, weight, offset, masks):
    rows = value.shape[0]
    ext[0:HALO, :] = halo
    ext[HALO : HALO + rows, :] = value
    out = offset + weight[0:1, :] * value
    moved = []
    for k in range(1, 4):
        shifted = ext[HALO - k : HALO - k + rows, :] * masks[k - 1]
        moved.append(shifted)
        out = out + weight[k : k + 1, :] * shifted
    return out, moved


def filter_back(ext, grad, later, weight, masks):
    rows = grad.shape[0]
    ext[0:rows, :] = grad
    ext[rows : rows + HALO, :] = later
    out = weight[0:1, :] * grad
    for k in range(1, 4):
        out = out + weight[k : k + 1, :] * (ext[k : k + rows, :] * masks[k - 1])
    return out


def block_pair(v):
    lane = lax.broadcasted_iota(jnp.int32, v.shape, 1)
    zero = jnp.zeros_like(v)
    return jnp.concatenate([jnp.where(lane < 64, v, zero), jnp.where(lane < 64, zero, v)], axis=0)


def forward_kernel(
    gate_ref, sig_ref, sigh_ref, mem_ref, memh_ref, step_ref, col_ref, row_ref, back_ref,
    kern_ref, off_ref, win_ref, shf_ref, base_ref, nrate_ref, short_ref, post_ref, ind_ref,
    y_ref, state_ref, stat_ref, held, ext, extm,
):
    rows = CHUNK
    inner = sig_ref.shape[1]
    pairs = inner // LANES

    @pl.when(pl.program_id(1) == 0)
    def _():
        held[...] = jnp.zeros_like(held)

    col = col_ref[...]
    masks = [col[:, k : k + 1] for k in range(3)]
    carried, keep, segc = col[:, 3:4], col[:, 4:5], col[:, 5:6]
    segr = row_ref[0:1, :]
    pre, _ = filtered(ext, sig_ref[...], sigh_ref[...], kern_ref[...], off_ref[...], masks)
    xs = pre * jax.nn.sigmoid(pre)
    prem, _ = filtered(extm, mem_ref[...], memh_ref[...], win_ref[...], shf_ref[...], masks)
    ms = prem * jax.nn.sigmoid(prem)
    writes, reads = ms[:, :LANES], ms[:, LANES:]
    step = softplus(step_ref[...] + base_ref[...])
    rate = nrate_ref[...] * step
    ti = lax.broadcasted_iota(jnp.int32, (rows, rows), 0)
    si = lax.broadcasted_iota(jnp.int32, (rows, rows), 1)
    tri = (si <= ti).astype(f32).astype(bf16)
    cum = tri_dot(tri, rate)
    cum2 = cum * LOG2E
    cum2_rows = cum2.T
    last = cum[rows - 1 : rows, :]
    enter = jnp.exp(cum) * carried
    toward = jnp.exp(last - cum) * keep
    once = ind_ref[0:LANES, :]
    twice = ind_ref[...]
    step_e = spread_heads(step, twice)
    enter_e = spread_heads(enter, twice)
    toward_e = spread_heads(toward, twice)
    scores = precise_nt(reads, writes)
    scores = jnp.where((si <= ti) & (segc == segr), scores, 0.0)
    u = step_e * xs
    ub = u.astype(bf16)
    state = held[...]
    state_ref[...] = state
    inter = dot_nn(reads.astype(bf16), state.astype(bf16))
    outs = []
    for j in range(pairs):
        parts = []
        for h in (2 * j, 2 * j + 1):
            fall = jnp.exp2(jnp.minimum(cum2[:, h : h + 1] - cum2_rows[h : h + 1, :], 0.0))
            parts.append((fall * scores).astype(bf16))
        upair = block_pair(ub[:, j * LANES : (j + 1) * LANES])
        outs.append(dot_nn(jnp.concatenate(parts, axis=1), upair))
    y = jnp.concatenate(outs, axis=1) + inter * enter_e + short_ref[...] * xs
    y_ref[...] = y
    held[...] = state * enter_e[rows - 1 : rows, :] + dot_nn(
        writes.T.astype(bf16), (toward_e * u).astype(bf16)
    )
    gate = gate_ref[...]
    gated = y * (gate * jax.nn.sigmoid(gate))
    squares = jnp.sum(gated * gated, axis=1, keepdims=True)
    dots = jnp.sum(gated * (back_ref[...] * post_ref[...]), axis=1, keepdims=True)
    lane = lax.broadcasted_iota(jnp.int32, (rows, LANES), 1)
    both = jnp.where(lane == 0, squares, jnp.where(lane == 1, dots, 0.0))
    stat_ref[...] = both.T[0:8, :]


def backward_kernel(
    gate_ref, sig_ref, sigh_ref, mem_ref, memh_ref, step_ref, col_ref, row_ref, back_ref,
    y_ref, fac_ref, state_ref,
    kern_ref, off_ref, win_ref, shf_ref, base_ref, nrate_ref, short_ref, post_ref, ind_ref,
    dgate_ref, dsig_ref, dmem_ref, dstep_ref, wide_ref, window_ref, head_ref,
    held, ext, extm, later, laterm,
):
    rows = CHUNK
    inner = sig_ref.shape[1]
    pairs = inner // LANES
    inv_inner = fac_ref[:, 2:3]

    @pl.when(pl.program_id(1) == 0)
    def _():
        held[...] = jnp.zeros_like(held)
        later[...] = jnp.zeros_like(later)
        laterm[...] = jnp.zeros_like(laterm)

    @pl.when((pl.program_id(0) == 0) & (pl.program_id(1) == 0))
    def _():
        wide_ref[...] = jnp.zeros_like(wide_ref)
        window_ref[...] = jnp.zeros_like(window_ref)
        head_ref[...] = jnp.zeros_like(head_ref)

    col = col_ref[...]
    masks = [col[:, k : k + 1] for k in range(3)]
    carried, keep, segc = col[:, 3:4], col[:, 4:5], col[:, 5:6]
    ahead = [col[:, k : k + 1] for k in range(6, 9)]
    segr = row_ref[0:1, :]

    factor = fac_ref[:, 0:1]
    gate = gate_ref[...]
    y = y_ref[...]
    back = back_ref[...]
    sg = jax.nn.sigmoid(gate)
    sl = gate * sg
    balanced = y * sl * factor
    grad = factor * (back * post_ref[...] - balanced * inv_inner)
    wide_ref[5:6, :] += jnp.sum(back * balanced, axis=0, keepdims=True)
    dy = grad * sl
    dgate_ref[...] = (grad * y * (sg * (1.0 + gate * (1.0 - sg)))).astype(bf16)

    kern = kern_ref[...]
    win = win_ref[...]
    pre, moved = filtered(ext, sig_ref[...], sigh_ref[...], kern, off_ref[...], masks)
    sp = jax.nn.sigmoid(pre)
    xs = pre * sp
    prem, movedm = filtered(extm, mem_ref[...], memh_ref[...], win, shf_ref[...], masks)
    spm = jax.nn.sigmoid(prem)
    ms = prem * spm
    writes, reads = ms[:, :LANES], ms[:, LANES:]
    shifted = step_ref[...] + base_ref[...]
    step = softplus(shifted)
    nrate = nrate_ref[...]
    rate = nrate * step
    si = lax.broadcasted_iota(jnp.int32, (rows, rows), 0)
    ti = lax.broadcasted_iota(jnp.int32, (rows, rows), 1)
    low = (ti <= si).astype(f32).astype(bf16)
    low_strict = (ti < si).astype(f32).astype(bf16)
    high = (ti >= si).astype(f32).astype(bf16)
    cum = tri_dot(low, rate)
    cum2 = cum * LOG2E
    cum2_rows = cum2.T
    last = cum[rows - 1 : rows, :]
    enter = jnp.exp(cum) * carried
    toward = jnp.exp(last - cum) * keep
    once = ind_ref[0:LANES, :]
    twice = ind_ref[...]
    step_e = spread_heads(step, twice)
    enter_e = spread_heads(enter, twice)
    toward_e = spread_heads(toward, twice)
    seg_row = segr
    inside = (si <= ti) & (segc == seg_row)
    scores = precise_nt(writes, reads)
    scores_in = jnp.where(inside, scores, 0.0)
    scores_strict = jnp.where(inside & (si < ti), scores, 0.0)
    u = step_e * xs
    ub = u.astype(bf16)
    dyb = dy.astype(bf16)
    state = state_ref[...]
    dstate = held[...]
    stateb = state.astype(bf16)
    dstateb = dstate.astype(bf16)
    rb = reads.astype(bf16)
    wb = writes.astype(bf16)

    dscore = jnp.zeros((rows, rows), f32)
    lane = lax.broadcasted_iota(jnp.int32, (rows, LANES), 1)
    as_source = jnp.zeros((rows, LANES), f32)
    as_target = []
    dus = []
    for j in range(pairs):
        dypair = block_pair(dyb[:, j * LANES : (j + 1) * LANES])
        cross = dot_nt(ub[:, j * LANES : (j + 1) * LANES], dypair)
        parts = []
        for i, h in enumerate((2 * j, 2 * j + 1)):
            fall = jnp.exp2(jnp.minimum(cum2_rows[h : h + 1, :] - cum2[:, h : h + 1], 0.0))
            parts.append((fall * scores_in).astype(bf16))
            weighted = fall * cross[:, i * rows : (i + 1) * rows]
            dscore = dscore + weighted
            flow = weighted * scores_strict
            as_source = jnp.where(lane == h, jnp.sum(flow, axis=1, keepdims=True), as_source)
            as_target.append(jnp.sum(flow, axis=0, keepdims=True))
        dus.append(dot_nn(jnp.concatenate(parts, axis=1), dypair))
    target = jnp.concatenate(
        as_target + [jnp.zeros((LANES - 2 * pairs, rows), f32)], axis=0
    ).T
    dscore = jnp.where(inside, dscore, 0.0)

    leaving = toward_e * dot_nn(wb, dstateb)
    du = jnp.concatenate(dus, axis=1) + leaving
    entered = enter_e * dy
    arriving = entered * dot_nn(rb, stateb)
    dx = short_ref[...] * dy + step_e * du
    dscore_b = dscore.astype(bf16)
    dwrites = dot_nn(dscore_b, rb) + dot_nt((toward_e * u).astype(bf16), dstateb)
    enteredb = entered.astype(bf16)
    dreads = dot_nn(dscore.T.astype(bf16), wb) + dot_nt(enteredb, stateb)
    persist_e = enter_e[rows - 1 : rows, :]
    across = jnp.sum(dstate * state, axis=0, keepdims=True) * persist_e
    held[...] = dstate * persist_e + dot_nn(reads.T.astype(bf16), enteredb)

    dstep_direct = sum_heads(xs * du, once)
    sent = sum_heads(u * leaving, once)
    got = sum_heads(arriving, once)
    across_h = sum_heads(jnp.broadcast_to(across, (8, inner)), once)[0:1, :]
    drate = tri_dot(high, got + target - as_source) + tri_dot(low_strict, sent) + across_h
    dstep = (nrate * drate + dstep_direct) * jax.nn.sigmoid(shifted)
    dstep_ref[...] = dstep.astype(bf16)
    head_ref[0:1, :] += jnp.sum(dstep, axis=0, keepdims=True)
    head_ref[1:2, :] += jnp.sum(drate * rate, axis=0, keepdims=True)
    wide_ref[6:7, :] += jnp.sum(dy * xs, axis=0, keepdims=True)

    dpre = dx * (sp * (1.0 + pre * (1.0 - sp)))
    dsig_ref[...] = filter_back(ext, dpre, later[...], kern, ahead).astype(bf16)
    later[...] = dpre[0:HALO, :]
    wide_ref[0:1, :] += jnp.sum(dpre * sig_ref[...], axis=0, keepdims=True)
    for k in range(3):
        wide_ref[k + 1 : k + 2, :] += jnp.sum(dpre * moved[k], axis=0, keepdims=True)
    wide_ref[4:5, :] += jnp.sum(dpre, axis=0, keepdims=True)
    dprem = jnp.concatenate([dwrites, dreads], axis=1) * (spm * (1.0 + prem * (1.0 - spm)))
    dmem_ref[...] = filter_back(extm, dprem, laterm[...], win, ahead).astype(bf16)
    laterm[...] = dprem[0:HALO, :]
    window_ref[0:1, :] += jnp.sum(dprem * mem_ref[...], axis=0, keepdims=True)
    for k in range(3):
        window_ref[k + 1 : k + 2, :] += jnp.sum(dprem * movedm[k], axis=0, keepdims=True)
    window_ref[4:5, :] += jnp.sum(dprem, axis=0, keepdims=True)


def full_spec(shape):
    return pl.BlockSpec(shape, lambda b, c: (0,) * len(shape))


def mixer_columns(segments):
    rows = segments.reshape(-1, SEQLEN)
    place = jnp.arange(SEQLEN, dtype=jnp.int32)[None, :]
    out = []
    for k in range(1, 4):
        earlier = jnp.roll(rows, k, axis=1)
        out.append((earlier == rows) & (place >= k))
    chunked = rows.reshape(rows.shape[0], SEQLEN // CHUNK, CHUNK)
    tail = chunked[:, :, -1]
    before = jnp.concatenate([jnp.full_like(tail[:, :1], -1), tail[:, :-1]], axis=1)
    out.append((chunked == before[:, :, None]).reshape(rows.shape))
    out.append((chunked == tail[:, :, None]).reshape(rows.shape))
    out.append(rows)
    for k in range(1, 4):
        ahead = jnp.roll(rows, -k, axis=1)
        out.append((ahead == rows) & (place < SEQLEN - k))
    cols = jnp.stack([member.reshape(-1).astype(f32) for member in out], axis=1)
    cols = jnp.pad(cols, ((0, 0), (0, 16 - cols.shape[1])))
    row = jnp.broadcast_to(segments.astype(f32)[None, :], (8, segments.shape[0]))
    return cols, row


def specs(inner, reverse):
    chunks = SEQLEN // CHUNK
    step = CHUNK // HALO

    def at(b, c):
        return b * chunks + (chunks - 1 - c if reverse else c)

    def tall(width):
        return pl.BlockSpec((CHUNK, width), lambda b, c: (at(b, c), 0))

    def halo(width):
        return pl.BlockSpec((HALO, width), lambda b, c: (jnp.maximum(at(b, c) * step - 1, 0), 0))

    flat = pl.BlockSpec((8, CHUNK), lambda b, c: (0, at(b, c)))
    data = [tall(inner), tall(inner), halo(inner), tall(2 * LANES), halo(2 * LANES), tall(LANES), tall(16), flat, tall(inner)]
    weights = [full_spec((4, inner)), full_spec((1, inner)), full_spec((4, 2 * LANES)), full_spec((1, 2 * LANES)), full_spec((1, LANES)), full_spec((1, LANES)), full_spec((1, inner)), full_spec((1, inner)), full_spec((2 * LANES, inner))]
    return tall, flat, data, weights


def mixer_forward(data, weights):
    tokens, inner = data[0].shape
    chunks = SEQLEN // CHUNK
    tall, flat, dspecs, wspecs = specs(inner, False)
    return pl.pallas_call(
        forward_kernel,
        grid=(tokens // SEQLEN, chunks),
        in_specs=dspecs + wspecs,
        out_specs=[tall(inner), tall(inner), flat],
        out_shape=[
            jax.ShapeDtypeStruct((tokens, inner), f32),
            jax.ShapeDtypeStruct((tokens, inner), f32),
            jax.ShapeDtypeStruct((8, tokens), f32),
        ],
        scratch_shapes=[
            pltpu.VMEM((LANES, inner), f32),
            pltpu.VMEM((CHUNK + HALO, inner), f32),
            pltpu.VMEM((CHUNK + HALO, 2 * LANES), f32),
        ],
        compiler_params=pltpu.CompilerParams(dimension_semantics=("arbitrary", "arbitrary"), vmem_limit_bytes=50 << 20),
        name="mixer_forward",
    )(*data, *weights)


def mixer_backward(data, y, fac, states, weights):
    tokens, inner = data[0].shape
    chunks = SEQLEN // CHUNK
    tall, flat, dspecs, wspecs = specs(inner, True)
    return pl.pallas_call(
        backward_kernel,
        grid=(tokens // SEQLEN, chunks),
        in_specs=dspecs + [tall(inner), tall(fac.shape[1]), tall(inner)] + wspecs,
        out_specs=[tall(inner), tall(inner), tall(2 * LANES), tall(LANES), full_spec((8, inner)), full_spec((8, 2 * LANES)), full_spec((8, LANES))],
        out_shape=[
            jax.ShapeDtypeStruct((tokens, inner), bf16),
            jax.ShapeDtypeStruct((tokens, inner), bf16),
            jax.ShapeDtypeStruct((tokens, 2 * LANES), bf16),
            jax.ShapeDtypeStruct((tokens, LANES), bf16),
            jax.ShapeDtypeStruct((8, inner), f32),
            jax.ShapeDtypeStruct((8, 2 * LANES), f32),
            jax.ShapeDtypeStruct((8, LANES), f32),
        ],
        scratch_shapes=[
            pltpu.VMEM((LANES, inner), f32),
            pltpu.VMEM((CHUNK + HALO, inner), f32),
            pltpu.VMEM((CHUNK + HALO, 2 * LANES), f32),
            pltpu.VMEM((HALO, inner), f32),
            pltpu.VMEM((HALO, 2 * LANES), f32),
        ],
        compiler_params=pltpu.CompilerParams(dimension_semantics=("arbitrary", "arbitrary"), vmem_limit_bytes=50 << 20),
        name="mixer_backward",
    )(*data, y, fac, states, *weights)


def contract_rows(left_side, right_side):
    return lax.dot_general(left_side, right_side, (((0,), (0,)), ((), ())), preferred_element_type=f32)


def local(
    tokens, segments, prenorm, gating, signal, memory, timestep, kernel, offsets, window, shifts,
    baseline, decays, shortcut, postnorm, readout, cotangent,
):
    width_here = tokens.shape[1]
    width = memory.shape[0]
    groups = width // width_here
    inner = gating.shape[1]
    whole = inner * groups
    heads = baseline.shape[0]
    position = lax.axis_index("tensor") * width_here
    gain_here = lax.dynamic_slice_in_dim(prenorm, position, width_here)
    tokens_wide = tokens.astype(f32)
    gathered = lax.all_gather(tokens, "tensor", axis=1, tiled=True)
    piece = lax.all_gather(cotangent, "tensor", axis=1, tiled=True)
    gathered_wide = gathered.astype(f32)
    inverse = lax.rsqrt(jnp.mean(gathered_wide * gathered_wide, axis=-1, keepdims=True) + epsilon)
    normed = (gathered_wide * inverse * prenorm).astype(bf16)
    scaled_rows = tokens_wide * inverse
    timestep_wide = jnp.pad(timestep, ((0, 0), (0, LANES - heads)))
    gate_in = jnp.dot(normed, gating, preferred_element_type=f32)
    signal_in = jnp.dot(normed, signal, preferred_element_type=f32)
    memory_in = jnp.dot(normed, memory, preferred_element_type=f32)
    step_in = jnp.dot(normed, timestep_wide, preferred_element_type=f32)
    back_rows = dot_nt(piece, readout)

    cols, row = mixer_columns(segments)
    head_width = inner // heads
    once = jnp.repeat(jnp.eye(LANES, heads, dtype=f32), head_width, axis=1).astype(bf16)
    pad = lambda v: jnp.pad(v[None, :], ((0, 0), (0, LANES - heads)))
    weights = (
        kernel, offsets[None, :], window, shifts[None, :], pad(baseline), pad(-jnp.exp(decays)),
        jnp.repeat(shortcut, head_width)[None, :], postnorm[None, :], jnp.concatenate([once, once], axis=0),
    )
    data = (gate_in, signal_in, signal_in, memory_in, memory_in, step_in, cols, row, back_rows)
    y, states, stat = mixer_forward(data, weights)
    sums = lax.psum(stat[0:2], "tensor")
    factor = lax.rsqrt(sums[0] / whole + epsilon)
    dots = sums[1] * factor
    fac = jnp.stack([factor, dots, dots / whole], axis=1)
    outnormed = (y * (gate_in * jax.nn.sigmoid(gate_in)) * factor[:, None] * postnorm).astype(bf16)
    readout_grad = contract_rows(outnormed, piece)
    readout_grad = lax.psum(readout_grad.astype(bf16), "dp")
    partial_out = jnp.dot(outnormed, readout, preferred_element_type=f32).astype(bf16)
    summed_out = lax.psum_scatter(partial_out, "tensor", scatter_dimension=1, tiled=True)
    outcome = (tokens_wide + summed_out.astype(f32)).astype(bf16)

    gate_low, signal_low, memory_low, step_low, wide, window_sums, head_sums = mixer_backward(
        data, y, fac, states, weights
    )
    gating_grad = contract_rows(normed, gate_low)
    gating_grad = lax.psum(gating_grad.astype(bf16), "dp")
    signal_grad = contract_rows(normed, signal_low)
    signal_grad = lax.psum(signal_grad.astype(bf16), "dp")
    normed_part = (
        dot_nt(gate_low, gating) + dot_nt(signal_low, signal)
        + dot_nt(step_low, timestep_wide) + dot_nt(memory_low, memory)
    )
    scaled_all = gathered_wide * inverse
    norm_dots = lax.psum(jnp.sum(normed_part * prenorm * scaled_all, axis=-1), "tensor")
    normed_back = lax.psum_scatter(normed_part.astype(bf16), "tensor", scatter_dimension=1, tiled=True).astype(f32)
    scaled_back = normed_back * gain_here
    prenorm_grad = jnp.sum(normed_back * scaled_rows, axis=0)
    tokens_grad = inverse * (scaled_back - scaled_rows * norm_dots[:, None] / width) + cotangent.astype(f32)

    timestep_grad = contract_rows(normed, step_low)[:, :heads]
    memory_grad = contract_rows(normed, memory_low)
    memory_grad = lax.psum_scatter(memory_grad, "tensor", scatter_dimension=0, tiled=True)
    window_sums = lax.psum(window_sums, ("dp", "tensor"))
    shortcut_grad = wide[6].reshape(heads, head_width).sum(axis=1)
    prenorm_grad, memory_grad, timestep_grad, wide, head_sums, shortcut_grad = lax.psum(
        (prenorm_grad, memory_grad, timestep_grad, wide[:6], head_sums[:2, :heads], shortcut_grad), "dp"
    )
    return (
        outcome, tokens_grad, prenorm_grad, gating_grad.astype(f32), signal_grad.astype(f32), memory_grad,
        timestep_grad, wide[0:4], wide[4], window_sums[0:4], window_sums[4], head_sums[0], head_sums[1],
        shortcut_grad, wide[5], readout_grad.astype(f32),
    )


def solution(mesh):
    placed = (
        P("dp", "tensor"), P("dp"), P(), P(None, "tensor"), P(None, "tensor"), P(), P(None, "tensor"),
        P(None, "tensor"), P("tensor"), P(), P(), P("tensor"), P("tensor"), P("tensor"), P("tensor"),
        P("tensor", None), P("dp", "tensor"),
    )
    return jax.shard_map(
        local,
        mesh=mesh,
        in_specs=placed,
        out_specs=(
            P("dp", "tensor"), P("dp", "tensor"), P("tensor"), P(None, "tensor"), P(None, "tensor"),
            P("tensor", None), P(None, "tensor"), P(None, "tensor"), P("tensor"), P(), P(), P("tensor"),
            P("tensor"), P("tensor"), P("tensor"), P("tensor", None),
        ),
        check_vma=False,
    )
```

```python
from functools import partial

import jax
import numpy as np
import jax.numpy as jnp
from jax import lax
from jax.experimental import pallas as pl
from jax.experimental.pallas import tpu as pltpu
from jax.sharding import PartitionSpec as P


SEQLEN = 1024
CHUNK = 128
LANES = 128
HALO = 8
LOG2E = 1.4426950408889634
epsilon = 1e-05
f32 = jnp.float32
bf16 = jnp.bfloat16


def dot_nn(a, b):
    return lax.dot_general(a, b, (((1,), (0,)), ((), ())), preferred_element_type=f32)


def dot_nt(a, b):
    return lax.dot_general(a, b, (((1,), (1,)), ((), ())), preferred_element_type=f32)


def halves(v):
    hi = v.astype(bf16)
    lo = (v - hi.astype(f32)).astype(bf16)
    return hi, lo


def spread_heads(v, twice):
    hi, lo = halves(v)
    return dot_nn(jnp.concatenate([hi, lo], axis=1), twice)


def sum_heads(v, once):
    hi, lo = halves(v)
    return dot_nt(hi, once) + dot_nt(lo, once)


def tri_dot(tri, v):
    hi = v.astype(bf16)
    rest = v - hi.astype(f32)
    mid = rest.astype(bf16)
    lo = (rest - mid.astype(f32)).astype(bf16)
    return dot_nn(tri, hi) + (dot_nn(tri, mid) + dot_nn(tri, lo))


def softplus(v):
    return jnp.maximum(v, 0.0) + jnp.log1p(jnp.exp(-jnp.abs(v)))


def precise_nt(a, b):
    ah, al = halves(a)
    bh, bl = halves(b)
    return dot_nt(jnp.concatenate([ah, ah, al], axis=1), jnp.concatenate([bh, bl, bh], axis=1))


def filtered(ext, value, halo, weight, offset, masks):
    rows = value.shape[0]
    ext[0:HALO, :] = halo
    ext[HALO : HALO + rows, :] = value
    out = offset + weight[0:1, :] * value
    moved = []
    for k in range(1, 4):
        shifted = ext[HALO - k : HALO - k + rows, :] * masks[k - 1]
        moved.append(shifted)
        out = out + weight[k : k + 1, :] * shifted
    return out, moved


def filter_back(ext, grad, later, weight, masks):
    rows = grad.shape[0]
    ext[0:rows, :] = grad
    ext[rows : rows + HALO, :] = later
    out = weight[0:1, :] * grad
    for k in range(1, 4):
        out = out + weight[k : k + 1, :] * (ext[k : k + rows, :] * masks[k - 1])
    return out


def segment_masks(col_ref, before_ref, after_ref, row_ref, segs, chunk):
    rows = CHUNK
    here = col_ref[...]
    segs[0:HALO, :] = jnp.where(chunk == 0, -1.0, before_ref[...])
    segs[HALO : HALO + rows, :] = here
    segs[HALO + rows :, :] = jnp.where(chunk == SEQLEN // CHUNK - 1, -1.0, after_ref[...])
    same = lambda k: (segs[HALO + k : HALO + k + rows, :] == here).astype(f32)
    carried = (here == segs[HALO - 1 : HALO, :]).astype(f32)
    keep = (here == segs[HALO + rows - 1 : HALO + rows, :]).astype(f32)
    return [same(-k) for k in (1, 2, 3)], [same(k) for k in (1, 2, 3)], carried, keep, here, row_ref[...]


def block_pair(v):
    lane = lax.broadcasted_iota(jnp.int32, v.shape, 1)
    zero = jnp.zeros_like(v)
    return jnp.concatenate([jnp.where(lane < 64, v, zero), jnp.where(lane < 64, zero, v)], axis=0)


def forward_kernel(
    gate_ref, sig_ref, sigh_ref, mem_ref, memh_ref, step_ref, col_ref, before_ref, after_ref, row_ref, back_ref,
    kern_ref, off_ref, win_ref, shf_ref, base_ref, nrate_ref, short_ref, post_ref, ind_ref,
    y_ref, state_ref, stat_ref, held, ext, extm, segs,
):
    rows = CHUNK
    inner = sig_ref.shape[1]
    pairs = inner // LANES

    @pl.when(pl.program_id(1) == 0)
    def _():
        held[...] = jnp.zeros_like(held)

    masks, _, carried, keep, segc, segr = segment_masks(col_ref, before_ref, after_ref, row_ref, segs, pl.program_id(1))
    pre, _ = filtered(ext, sig_ref[...], sigh_ref[...], kern_ref[...], off_ref[...], masks)
    xs = pre * jax.nn.sigmoid(pre)
    prem, _ = filtered(extm, mem_ref[...], memh_ref[...], win_ref[...], shf_ref[...], masks)
    ms = prem * jax.nn.sigmoid(prem)
    writes, reads = ms[:, :LANES], ms[:, LANES:]
    step = softplus(step_ref[...] + base_ref[...])
    rate = nrate_ref[...] * step
    ti = lax.broadcasted_iota(jnp.int32, (rows, rows), 0)
    si = lax.broadcasted_iota(jnp.int32, (rows, rows), 1)
    tri = (si <= ti).astype(f32).astype(bf16)
    cum = tri_dot(tri, rate)
    cum2 = cum * LOG2E
    cum2_rows = cum2.T
    last = cum[rows - 1 : rows, :]
    enter = jnp.exp(cum) * carried
    toward = jnp.exp(last - cum) * keep
    twice = ind_ref[...]
    step_e = spread_heads(step, twice)
    enter_e = spread_heads(enter, twice)
    toward_e = spread_heads(toward, twice)
    scores = precise_nt(reads, writes)
    scores = jnp.where((si <= ti) & (segc == segr), scores, 0.0)
    u = step_e * xs
    ub = u.astype(bf16)
    state = held[...]
    state_ref[...] = state
    inter = dot_nn(reads.astype(bf16), state.astype(bf16))
    outs = []
    for j in range(pairs):
        parts = []
        for h in (2 * j, 2 * j + 1):
            fall = jnp.exp2(jnp.minimum(cum2[:, h : h + 1] - cum2_rows[h : h + 1, :], 0.0))
            parts.append((fall * scores).astype(bf16))
        upair = block_pair(ub[:, j * LANES : (j + 1) * LANES])
        outs.append(dot_nn(jnp.concatenate(parts, axis=1), upair))
    y = jnp.concatenate(outs, axis=1) + inter * enter_e + short_ref[...] * xs
    y_ref[...] = y
    held[...] = state * enter_e[rows - 1 : rows, :] + dot_nn(
        writes.T.astype(bf16), (toward_e * u).astype(bf16)
    )
    gate = gate_ref[...]
    gated = y * (gate * jax.nn.sigmoid(gate))
    squares = jnp.sum(gated * gated, axis=1, keepdims=True)
    dots = jnp.sum(gated * (back_ref[...] * post_ref[...]), axis=1, keepdims=True)
    lane = lax.broadcasted_iota(jnp.int32, (rows, LANES), 1)
    both = jnp.where(lane == 0, squares, jnp.where(lane == 1, dots, 0.0))
    stat_ref[...] = both.T[0:8, :]


def backward_kernel(
    dy_ref, sig_ref, sigh_ref, mem_ref, memh_ref, step_ref, col_ref, before_ref, after_ref, row_ref, state_ref,
    kern_ref, off_ref, win_ref, shf_ref, base_ref, nrate_ref, short_ref, ind_ref,
    dsig_ref, dmem_ref, dstep_ref, wide_ref, window_ref, head_ref,
    held, ext, extm, segs, later, laterm,
):
    rows = CHUNK
    inner = sig_ref.shape[1]
    pairs = inner // LANES

    @pl.when(pl.program_id(1) == 0)
    def _():
        held[...] = jnp.zeros_like(held)
        later[...] = jnp.zeros_like(later)
        laterm[...] = jnp.zeros_like(laterm)

        wide_ref[...] = jnp.zeros_like(wide_ref)
        window_ref[...] = jnp.zeros_like(window_ref)
        head_ref[...] = jnp.zeros_like(head_ref)

    masks, ahead, carried, keep, segc, segr = segment_masks(
        col_ref, before_ref, after_ref, row_ref, segs, pl.num_programs(1) - 1 - pl.program_id(1)
    )

    dy = dy_ref[...]

    kern = kern_ref[...]
    win = win_ref[...]
    pre, moved = filtered(ext, sig_ref[...], sigh_ref[...], kern, off_ref[...], masks)
    sp = jax.nn.sigmoid(pre)
    xs = pre * sp
    prem, movedm = filtered(extm, mem_ref[...], memh_ref[...], win, shf_ref[...], masks)
    spm = jax.nn.sigmoid(prem)
    ms = prem * spm
    writes, reads = ms[:, :LANES], ms[:, LANES:]
    shifted = step_ref[...] + base_ref[...]
    step = softplus(shifted)
    nrate = nrate_ref[...]
    rate = nrate * step
    si = lax.broadcasted_iota(jnp.int32, (rows, rows), 0)
    ti = lax.broadcasted_iota(jnp.int32, (rows, rows), 1)
    low = (ti <= si).astype(f32).astype(bf16)
    low_strict = (ti < si).astype(f32).astype(bf16)
    high = (ti >= si).astype(f32).astype(bf16)
    cum = tri_dot(low, rate)
    cum2 = cum * LOG2E
    cum2_rows = cum2.T
    last = cum[rows - 1 : rows, :]
    enter = jnp.exp(cum) * carried
    toward = jnp.exp(last - cum) * keep
    once = ind_ref[0:LANES, :]
    twice = ind_ref[...]
    step_e = spread_heads(step, twice)
    enter_e = spread_heads(enter, twice)
    toward_e = spread_heads(toward, twice)
    seg_row = segr
    inside = (si <= ti) & (segc == seg_row)
    scores = precise_nt(writes, reads)
    scores_in = jnp.where(inside, scores, 0.0)
    scores_strict = jnp.where(inside & (si < ti), scores, 0.0)
    u = step_e * xs
    ub = u.astype(bf16)
    dyb = dy.astype(bf16)
    state = state_ref[...]
    dstate = held[...]
    stateb = state.astype(bf16)
    dstateb = dstate.astype(bf16)
    rb = reads.astype(bf16)
    wb = writes.astype(bf16)

    dscore = jnp.zeros((rows, rows), f32)
    lane = lax.broadcasted_iota(jnp.int32, (rows, LANES), 1)
    as_source = jnp.zeros((rows, LANES), f32)
    as_target = []
    dus = []
    for j in range(pairs):
        dypair = block_pair(dyb[:, j * LANES : (j + 1) * LANES])
        cross = dot_nt(ub[:, j * LANES : (j + 1) * LANES], dypair)
        parts = []
        for i, h in enumerate((2 * j, 2 * j + 1)):
            fall = jnp.exp2(jnp.minimum(cum2_rows[h : h + 1, :] - cum2[:, h : h + 1], 0.0))
            parts.append((fall * scores_in).astype(bf16))
            weighted = fall * cross[:, i * rows : (i + 1) * rows]
            dscore = dscore + weighted
            flow = weighted * scores_strict
            as_source = jnp.where(lane == h, jnp.sum(flow, axis=1, keepdims=True), as_source)
            as_target.append(jnp.sum(flow, axis=0, keepdims=True))
        dus.append(dot_nn(jnp.concatenate(parts, axis=1), dypair))
    target = jnp.concatenate(
        as_target + [jnp.zeros((LANES - 2 * pairs, rows), f32)], axis=0
    ).T
    dscore = jnp.where(inside, dscore, 0.0)

    leaving = toward_e * dot_nn(wb, dstateb)
    du = jnp.concatenate(dus, axis=1) + leaving
    entered = enter_e * dy
    arriving = entered * dot_nn(rb, stateb)
    dx = short_ref[...] * dy + step_e * du
    dscore_b = dscore.astype(bf16)
    dwrites = dot_nn(dscore_b, rb) + dot_nt((toward_e * u).astype(bf16), dstateb)
    enteredb = entered.astype(bf16)
    dreads = dot_nn(dscore.T.astype(bf16), wb) + dot_nt(enteredb, stateb)
    persist_e = enter_e[rows - 1 : rows, :]
    across = jnp.sum(dstate * state, axis=0, keepdims=True) * persist_e
    held[...] = dstate * persist_e + dot_nn(reads.T.astype(bf16), enteredb)

    dstep_direct = sum_heads(xs * du, once)
    sent = sum_heads(u * leaving, once)
    got = sum_heads(arriving, once)
    across_h = sum_heads(jnp.broadcast_to(across, (8, inner)), once)[0:1, :]
    drate = tri_dot(high, got + target - as_source) + tri_dot(low_strict, sent) + across_h
    dstep = (nrate * drate + dstep_direct) * jax.nn.sigmoid(shifted)
    dstep_ref[...] = dstep.astype(bf16)
    head_ref[0:1, :] += jnp.sum(dstep, axis=0, keepdims=True)
    head_ref[1:2, :] += jnp.sum(drate * rate, axis=0, keepdims=True)
    wide_ref[5:6, :] += jnp.sum(dy * xs, axis=0, keepdims=True)

    dpre = dx * (sp * (1.0 + pre * (1.0 - sp)))
    dsig_ref[...] = filter_back(ext, dpre, later[...], kern, ahead).astype(bf16)
    later[...] = dpre[0:HALO, :]
    wide_ref[0:1, :] += jnp.sum(dpre * sig_ref[...], axis=0, keepdims=True)
    for k in range(3):
        wide_ref[k + 1 : k + 2, :] += jnp.sum(dpre * moved[k], axis=0, keepdims=True)
    wide_ref[4:5, :] += jnp.sum(dpre, axis=0, keepdims=True)
    dprem = jnp.concatenate([dwrites, dreads], axis=1) * (spm * (1.0 + prem * (1.0 - spm)))
    dmem_ref[...] = filter_back(extm, dprem, laterm[...], win, ahead).astype(bf16)
    laterm[...] = dprem[0:HALO, :]
    window_ref[0:1, :] += jnp.sum(dprem * mem_ref[...], axis=0, keepdims=True)
    for k in range(3):
        window_ref[k + 1 : k + 2, :] += jnp.sum(dprem * movedm[k], axis=0, keepdims=True)
    window_ref[4:5, :] += jnp.sum(dprem, axis=0, keepdims=True)


def middle_kernel(whole, gate_ref, y_ref, back_ref, stat_ref, post_ref, out_ref, dgate_ref, dy_ref, sums_ref):
    @pl.when(pl.program_id(0) == 0)
    def _():
        sums_ref[...] = jnp.zeros_like(sums_ref)

    squares, dots = stat_ref[0:1, :], stat_ref[1:2, :]
    factor = lax.rsqrt(squares / whole + epsilon)
    dots = dots * factor / whole
    blank = jnp.zeros((LANES - 2, factor.shape[1]), f32)
    tall = jnp.concatenate([factor, dots, blank], axis=0).T
    factor, dots = tall[:, 0:1], tall[:, 1:2]
    gate = gate_ref[...]
    y = y_ref[...]
    back = back_ref[...]
    post = post_ref[...]
    sg = jax.nn.sigmoid(gate)
    sl = gate * sg
    balanced = y * sl * factor
    out_ref[...] = (balanced * post).astype(bf16)
    grad = factor * (back * post - balanced * dots)
    sums_ref[0:1, :] += jnp.sum(back * balanced, axis=0, keepdims=True)
    dy_ref[...] = grad * sl
    dgate_ref[...] = (grad * y * (sg * (1.0 + gate * (1.0 - sg)))).astype(bf16)


def norm_kernel(mine_ref, near_ref, far_ref, gain_ref, normed_ref, inv_ref):
    wide = jnp.concatenate([far_ref[...], near_ref[...], mine_ref[...]], axis=1).astype(f32)
    inverse = lax.rsqrt(jnp.mean(wide * wide, axis=1, keepdims=True) + epsilon)
    inv_ref[...] = inverse
    normed_ref[...] = (wide * inverse * gain_ref[...]).astype(bf16)


def inputs_kernel(
    dgate_ref, dsig_ref, dmem_ref, dstep_ref, mine_ref, near_ref, far_ref, inv_ref, gain_ref,
    gating_ref, signal_ref, memory_ref, timestep_ref, send_ref, keep_ref, dots_ref, sums_ref,
):
    @pl.when(pl.program_id(0) == 0)
    def _():
        sums_ref[...] = jnp.zeros_like(sums_ref)

    part = (
        dot_nt(dgate_ref[...], gating_ref[...]) + dot_nt(dsig_ref[...], signal_ref[...])
        + dot_nt(dmem_ref[...], memory_ref[...]) + dot_nt(dstep_ref[...], timestep_ref[...])
    )
    half = part.shape[1] // 2
    send_ref[...] = part[:, :half].astype(bf16)
    keep_ref[...] = part[:, half:]
    wide = jnp.concatenate([far_ref[...], near_ref[...], mine_ref[...]], axis=1).astype(f32)
    flow = part * (wide * inv_ref[...])
    sums_ref[0:1, :] += jnp.sum(flow, axis=0, keepdims=True)
    dots = jnp.sum(flow * gain_ref[...], axis=1, keepdims=True)
    dots_ref[...] = jnp.broadcast_to(dots, (dots.shape[0], LANES)).T[0:8, :]


def full_spec(shape):
    return pl.BlockSpec(shape, lambda *_: (0,) * len(shape))


def cost(flops, moved):
    return pl.CostEstimate(flops=int(flops), bytes_accessed=int(moved), transcendentals=0)


def params(axes):
    return pltpu.CompilerParams(dimension_semantics=("arbitrary",) * axes, vmem_limit_bytes=50 << 20)


def specs(inner, reverse):
    chunks = SEQLEN // CHUNK
    step = CHUNK // HALO

    def at(b, c):
        return b * chunks + (chunks - 1 - c if reverse else c)

    def tall(width):
        return pl.BlockSpec((CHUNK, width), lambda b, c: (at(b, c), 0))

    def halo(width):
        return pl.BlockSpec((HALO, width), lambda b, c: (jnp.maximum(at(b, c) * step - 1, 0), 0))

    def halo_after(width):
        last = SEQLEN // HALO - 1
        return pl.BlockSpec((HALO, width), lambda b, c: (jnp.minimum((at(b, c) + 1) * step, (b + 1) * (last + 1) - 1), 0))

    flat = pl.BlockSpec((8, CHUNK), lambda b, c: (0, at(b, c)))
    line = pl.BlockSpec((1, CHUNK), lambda b, c: (0, at(b, c)))
    data = [tall(inner), tall(inner), halo(inner), tall(2 * LANES), halo(2 * LANES), tall(LANES), tall(1), halo(1), halo_after(1), line]
    weights = [
        full_spec((4, inner)), full_spec((1, inner)), full_spec((4, 2 * LANES)), full_spec((1, 2 * LANES)),
        full_spec((1, LANES)), full_spec((1, LANES)), full_spec((1, inner)),
    ]
    return tall, flat, data, weights


def mixer_forward(data, back, weights, post, twice):
    tokens, inner = data[0].shape
    tall, flat, dspecs, wspecs = specs(inner, False)
    return pl.pallas_call(
        forward_kernel,
        grid=(tokens // SEQLEN, SEQLEN // CHUNK),
        in_specs=dspecs + [tall(inner)] + wspecs + [full_spec(post.shape), full_spec(twice.shape)],
        out_specs=[tall(inner), tall(inner), flat],
        out_shape=[
            jax.ShapeDtypeStruct((tokens, inner), f32),
            jax.ShapeDtypeStruct((tokens, inner), f32),
            jax.ShapeDtypeStruct((8, tokens), f32),
        ],
        scratch_shapes=[
            pltpu.VMEM((LANES, inner), f32),
            pltpu.VMEM((CHUNK + HALO, inner), f32),
            pltpu.VMEM((CHUNK + HALO, 2 * LANES), f32),
            pltpu.VMEM((CHUNK + 2 * HALO, 1), f32),
        ],
        compiler_params=params(2),
        cost_estimate=cost(8e9, 20e6),
        name="mixer_forward",
    )(*data, back, *weights, post, twice)


def mixer_backward(data, states, weights, twice):
    tokens, inner = data[0].shape
    tall, _, dspecs, wspecs = specs(inner, True)
    return pl.pallas_call(
        backward_kernel,
        grid=(tokens // SEQLEN, SEQLEN // CHUNK),
        in_specs=dspecs + [tall(inner)] + wspecs + [full_spec(twice.shape)],
        out_specs=[tall(inner), tall(2 * LANES), tall(LANES), full_spec((8, inner)), full_spec((8, 2 * LANES)), full_spec((8, LANES))],
        out_shape=[
            jax.ShapeDtypeStruct((tokens, inner), bf16),
            jax.ShapeDtypeStruct((tokens, 2 * LANES), bf16),
            jax.ShapeDtypeStruct((tokens, LANES), bf16),
            jax.ShapeDtypeStruct((8, inner), f32),
            jax.ShapeDtypeStruct((8, 2 * LANES), f32),
            jax.ShapeDtypeStruct((8, LANES), f32),
        ],
        scratch_shapes=[
            pltpu.VMEM((LANES, inner), f32),
            pltpu.VMEM((CHUNK + HALO, inner), f32),
            pltpu.VMEM((CHUNK + HALO, 2 * LANES), f32),
            pltpu.VMEM((CHUNK + 2 * HALO, 1), f32),
            pltpu.VMEM((HALO, inner), f32),
            pltpu.VMEM((HALO, 2 * LANES), f32),
        ],
        compiler_params=params(2),
        cost_estimate=cost(20e9, 40e6),
        name="mixer_backward",
    )(*data, states, *weights, twice)


def tall_spec(rows, width):
    return pl.BlockSpec((rows, width), lambda r: (r, 0))


def middle(gate, y, back, stat, post, whole):
    tokens, inner = y.shape
    rows = 256
    return pl.pallas_call(
        partial(middle_kernel, whole),
        grid=(tokens // rows,),
        in_specs=[tall_spec(rows, inner)] * 3 + [pl.BlockSpec((8, rows), lambda r: (0, r)), full_spec((1, inner))],
        out_specs=[tall_spec(rows, inner)] * 3 + [full_spec((8, inner))],
        out_shape=[
            jax.ShapeDtypeStruct((tokens, inner), bf16),
            jax.ShapeDtypeStruct((tokens, inner), bf16),
            jax.ShapeDtypeStruct((tokens, inner), f32),
            jax.ShapeDtypeStruct((8, inner), f32),
        ],
        compiler_params=params(1),
        cost_estimate=cost(1e8, 16e6),
        name="middle",
    )(gate, y, back, stat, post)


def norm(mine, near, far, gain):
    tokens, part = mine.shape
    width = 4 * part
    rows = 256
    return pl.pallas_call(
        norm_kernel,
        grid=(tokens // rows,),
        in_specs=[tall_spec(rows, part), tall_spec(rows, part), tall_spec(rows, 2 * part), full_spec((1, width))],
        out_specs=[tall_spec(rows, width), tall_spec(rows, 1)],
        out_shape=[jax.ShapeDtypeStruct((tokens, width), bf16), jax.ShapeDtypeStruct((tokens, 1), f32)],
        compiler_params=params(1),
        cost_estimate=cost(1e8, 7e6),
        name="norm",
    )(mine, near, far, gain)


def inputs_back(lows, mine, near, far, inverse, gain, weights):
    tokens, part = mine.shape
    width = 4 * part
    rows = 256
    return pl.pallas_call(
        inputs_kernel,
        grid=(tokens // rows,),
        in_specs=[tall_spec(rows, v.shape[1]) for v in lows]
        + [tall_spec(rows, part), tall_spec(rows, part), tall_spec(rows, 2 * part), tall_spec(rows, 1), full_spec((1, width))]
        + [full_spec(w.shape) for w in weights],
        out_specs=[
            tall_spec(rows, width // 2), tall_spec(rows, width // 2),
            pl.BlockSpec((8, rows), lambda r: (0, r)), full_spec((8, width)),
        ],
        out_shape=[
            jax.ShapeDtypeStruct((tokens, width // 2), bf16),
            jax.ShapeDtypeStruct((tokens, width // 2), f32),
            jax.ShapeDtypeStruct((8, tokens), f32),
            jax.ShapeDtypeStruct((8, width), f32),
        ],
        compiler_params=params(1),
        cost_estimate=cost(6e9, 16e6),
        name="inputs_back",
    )(*lows, mine, near, far, inverse, gain, *weights)


def flipped(value, axis, size, bits):
    return lax.ppermute(value, axis, [(i, i ^ bits) for i in range(size)])


def radices(size):
    assert size & (size - 1) == 0
    out = []
    stride = 1
    while stride < size:
        radix = 2 if not out else min(4, size // stride)
        out.append((radix, stride))
        stride *= radix
    return out


def reduce_stage(value, index, size, radix, stride):
    digit = (index // stride) % radix
    rows = value.shape[0] // radix
    total = lax.dynamic_slice_in_dim(value, digit * rows, rows).astype(f32)
    for k in range(1, radix):
        sent = lax.dynamic_slice_in_dim(value, (digit ^ k) * rows, rows).astype(bf16)
        total = total + flipped(sent, "dp", size, k * stride).astype(f32)
    return total


def gather_stage(value, index, size, radix, stride):
    digit = (index // stride) % radix
    pieces = [value] + [flipped(value, "dp", size, k * stride) for k in range(1, radix)]
    bit = 1
    while bit < radix:
        swap = (digit & bit) != 0
        pieces = [jnp.where(swap, pieces[k ^ bit], pieces[k]) for k in range(radix)]
        bit *= 2
    return jnp.concatenate(pieces, axis=0)


def sum_dp(value, index, size):
    stages = radices(size)
    for radix, stride in stages:
        value = reduce_stage(value, index, size, radix, stride)
    value = value.astype(bf16)
    for radix, stride in reversed(stages):
        value = gather_stage(value, index, size, radix, stride)
    return value


def sum_tensor(value):
    value = value + flipped(value, "tensor", 4, 1)
    return value + flipped(value, "tensor", 4, 2)


def share(mine):
    near = flipped(mine, "tensor", 4, 2)
    far = flipped(jnp.concatenate([near, mine], axis=1), "tensor", 4, 1)
    return near, far


def scatter_tensor(send, keep, axis):
    held = keep + flipped(send, "tensor", 4, 1).astype(f32)
    part = held.shape[axis] // 2
    sent = lax.slice_in_dim(held, 0, part, axis=axis).astype(bf16)
    return lax.slice_in_dim(held, part, 2 * part, axis=axis) + flipped(sent, "tensor", 4, 2).astype(f32)


def contract_rows(left_side, right_side):
    return lax.dot_general(left_side, right_side, (((0,), (0,)), ((), ())), preferred_element_type=f32)


def local(
    tokens, segments, prenorm, gating, signal, memory, timestep, kernel, offsets, window, shifts,
    baseline, decays, shortcut, postnorm, readout, cotangent,
):
    groups = lax.axis_size("tensor")
    assert groups == 4
    size = lax.axis_size("dp")
    dp = lax.axis_index("dp")
    me = lax.axis_index("tensor")
    width = memory.shape[0]
    part = width // groups
    inner = gating.shape[1]
    whole = inner * groups
    heads = baseline.shape[0]
    head_width = inner // heads
    sequences = tokens.shape[0] // SEQLEN
    order = [me ^ 3, me ^ 1, me ^ 2, me]

    def sorted_blocks(value, axis):
        return jnp.concatenate([lax.dynamic_slice_in_dim(value, b * part, part, axis) for b in order], axis=axis)

    def plain_blocks(value, axis):
        return jnp.concatenate(
            [lax.dynamic_slice_in_dim(value, slot * part, part, axis) for slot in [place_of(b) for b in range(4)]], axis=axis
        )

    def place_of(block):
        apart = block ^ me
        return 3 - jnp.where(apart == 1, 2, jnp.where(apart == 2, 1, apart))

    rows_of = lambda v, s: v[s * SEQLEN : (s + 1) * SEQLEN]
    token_parts, piece_parts = [], []
    for s in range(sequences):
        mine = rows_of(tokens, s)
        token_parts.append((mine,) + share(mine))
        mine = rows_of(cotangent, s)
        near, far = share(mine)
        piece_parts.append(jnp.concatenate([far, near, mine], axis=1))

    gain = sorted_blocks(prenorm[None, :], 1)
    gating_s, signal_s, memory_s = (sorted_blocks(w, 0) for w in (gating, signal, memory))
    timestep_s = sorted_blocks(jnp.pad(timestep, ((0, 0), (0, LANES - heads))), 0)
    readout_s = sorted_blocks(readout, 1)
    seg_wide = segments.astype(f32)
    seg_col, seg_row = seg_wide[:, None], seg_wide[None, :]
    once = np.repeat(np.eye(LANES, heads, dtype=np.float32), head_width, axis=1)
    twice = jnp.asarray(np.concatenate([once, once], axis=0), dtype=bf16)
    pad = lambda v: jnp.pad(v[None, :], ((0, 0), (0, LANES - heads)))
    post = postnorm[None, :]
    weights = (
        kernel, offsets[None, :], window, shifts[None, :], pad(baseline), pad(-jnp.exp(decays)),
        jnp.repeat(shortcut, head_width)[None, :],
    )

    project = lambda v, w: jnp.dot(v, w, preferred_element_type=f32)
    held = []
    for s in range(sequences):
        normed, inverse = norm(*token_parts[s], gain)
        gate_in = project(normed, gating_s)
        signal_in = project(normed, signal_s)
        memory_in = project(normed, memory_s)
        step_in = project(normed, timestep_s)
        back_rows = dot_nt(piece_parts[s], readout_s)
        col = rows_of(seg_col, s)
        data = (signal_in, signal_in, memory_in, memory_in, step_in, col, col, col, seg_row[:, s * SEQLEN : (s + 1) * SEQLEN])
        y, states, stat = mixer_forward((gate_in,) + data, back_rows, weights, post, twice)
        sums = sum_tensor(stat)
        held.append((normed, inverse, gate_in, back_rows, data, y, states, sums))

    outs, post_sums = [], 0.0
    for s in range(sequences):
        normed, inverse, gate_in, back_rows, data, y, states, sums = held[s]
        outnormed, gate_low, dy, post_sum = middle(gate_in, y, back_rows, sums, post, whole)
        post_sums = post_sums + post_sum[0]
        outs.append((outnormed, gate_low, dy))

    def weight_grad(left, right):
        total = 0.0
        for a, b in zip(left, right):
            total = total + contract_rows(a, b)
        return total.astype(bf16)

    normeds = [h[0] for h in held]
    readout_grad = weight_grad([o[0] for o in outs], piece_parts)
    gating_grad = weight_grad(normeds, [o[1] for o in outs])
    readout_sum = sum_dp(readout_grad, dp, size)
    gating_sum = sum_dp(gating_grad, dp, size)

    outcomes = []
    for s in range(sequences):
        outnormed = outs[s][0]
        send = project(outnormed, readout_s[:, : 2 * part]).astype(bf16)
        keep = project(outnormed, readout_s[:, 2 * part :])
        outcomes.append((rows_of(tokens, s).astype(f32) + scatter_tensor(send, keep, 1)).astype(bf16))

    lows, wide, window_sums, head_sums = [], 0.0, 0.0, 0.0
    for s in range(sequences):
        normed, inverse, gate_in, back_rows, data, y, states, sums = held[s]
        signal_low, memory_low, step_low, wide_s, window_s, head_s = mixer_backward(
            (outs[s][2],) + data, states, weights, twice
        )
        lows.append((outs[s][1], signal_low, memory_low, step_low))
        wide, window_sums, head_sums = wide + wide_s, window_sums + window_s, head_sums + head_s
    signal_grad = weight_grad(normeds, [v[1] for v in lows])
    signal_sum = sum_dp(signal_grad, dp, size)

    tokens_grads, gain_sums = [], 0.0
    for s in range(sequences):
        inverse = held[s][1]
        send, keep, dots, sums = inputs_back(
            lows[s], *token_parts[s], inverse, gain, (gating_s, signal_s, memory_s, timestep_s)
        )
        gain_sums = gain_sums + sums[0]
        dots = sum_tensor(dots)[0]
        scaled_back = scatter_tensor(send, keep, 1) * gain[:, 3 * part :]
        scaled = rows_of(tokens, s).astype(f32) * inverse
        tokens_grads.append(
            inverse * (scaled_back - scaled * (dots[:, None] / width)) + rows_of(cotangent, s).astype(f32)
        )

    window_sums = sum_tensor(window_sums)
    memory_grad = weight_grad(normeds, [v[2] for v in lows])
    timestep_grad = weight_grad(normeds, [v[3] for v in lows])[:, :heads]
    extra = jnp.pad(gain_sums[:, None], ((0, 0), (0, LANES - 1))).astype(bf16)
    both = jnp.concatenate([memory_grad, extra], axis=1)
    both = scatter_tensor(both[: 2 * part], both[2 * part :].astype(f32), 0)
    shortcut_grad = wide[5].reshape(heads, head_width).sum(axis=1)
    small = [
        both, timestep_grad.astype(f32), wide[0:5], post_sums, window_sums[0:5], head_sums[0:2, :heads], shortcut_grad,
    ]
    flat = jnp.concatenate([v.reshape(-1) for v in small])
    count = flat.shape[0]
    lines = 16 * size
    flat = jnp.pad(flat, (0, -count % (lines * LANES))).reshape(lines, -1)
    flat = sum_dp(flat, dp, size).astype(f32).reshape(-1)
    done, start = [], 0
    for v in small:
        done.append(flat[start : start + v.size].reshape(v.shape))
        start += v.size
    both, timestep_grad, wide, post_sums, window_sums, head_sums, shortcut_grad = done
    return (
        jnp.concatenate(outcomes, axis=0), jnp.concatenate(tokens_grads, axis=0), both[:, memory.shape[1]],
        plain_blocks(gating_sum, 0).astype(f32), plain_blocks(signal_sum, 0).astype(f32), both[:, : memory.shape[1]],
        plain_blocks(timestep_grad, 0), wide[0:4], wide[4], window_sums[0:4], window_sums[4], head_sums[0], head_sums[1],
        shortcut_grad, post_sums, plain_blocks(readout_sum, 1).astype(f32),
    )


def solution(mesh):
    placed = (
        P("dp", "tensor"), P("dp"), P(), P(None, "tensor"), P(None, "tensor"), P(), P(None, "tensor"),
        P(None, "tensor"), P("tensor"), P(), P(), P("tensor"), P("tensor"), P("tensor"), P("tensor"),
        P("tensor", None), P("dp", "tensor"),
    )

    return jax.shard_map(
        local,
        mesh=mesh,
        in_specs=placed,
        out_specs=(
            P("dp", "tensor"), P("dp", "tensor"), P("tensor"), P(None, "tensor"), P(None, "tensor"),
            P("tensor", None), P(None, "tensor"), P(None, "tensor"), P("tensor"), P(), P(), P("tensor"),
            P("tensor"), P("tensor"), P("tensor"), P("tensor", None),
        ),
        check_vma=False,
    )
```
